32 devices in a mesh: patch: 8 (over y, x, core), rhs: 4 (over z).
Axes of the slice: x: 2, y: 2, z: 4, core: 2. Of those that a mesh axis runs over, the one named last changes fastest.
Arguments:
- rhs_vectors: float32 [64, 16, 384], P('patch', 'rhs'), may hold values from -8 to 8
- near_blocks: bfloat16 [64, 4, 384, 384], P('patch'), may hold values from -1 to 5, as said below
- neighbours: int32 [64, 4], P('patch'), may hold values from 0 to 63, as said below
- up_maps: float32 [64, 64, 384], P('patch'), may hold values from -0.3125 to 0.3125
- shift_up: float32 [64, 64, 64], P('patch'), may hold values from -0.25 to 0.25
- far_lists: int32 [8, 4], P('patch'), may hold values from 0 to 7, as said below
- translations: float32 [8, 4, 64, 64], P('patch'), may hold values from -0.375 to 0.375
- shift_down: float32 [64, 64, 64], P('patch'), may hold values from -0.75 to 0.75
- down_maps: float32 [64, 384, 64], P('patch'), may hold values from -0.375 to 0.375
Outputs:
- solution: float32 [64, 16, 384], P('patch', 'rhs')
- residual: float32 [64, 16, 384], P('patch', 'rhs')
The draws below stay inside these ranges and needn't reach their ends.
Inputs may be any that keep to these rules, and one draw needn't show every extreme that they name: `neighbours`: entry 0 of each row is the patch itself; every other entry names a patch of the same cell or of the cell just before or just after it, cyclically. `far_lists`: entry 0 of each row names the cell just before or just after the row's own cell, cyclically, and for cell 0 the cell just before it; every other entry names a cell other than the row's own. `near_blocks`: the blocks keep the operator's symmetric part positive definite.
All inputs are finite; a program needn't handle non-finite values.
Results may differ from the reference program's by a relative error of at most 0.008.
The reference program's roundings to bfloat16 on the way (of `rounded`) count: a program that leaves them out, or rounds other values in their place, can miss the bound.
Values may be sent and summed in bfloat16 or wider, within the bound.
A program may use at most 64 MiB of HBM per device.

```python
import math
import jax
import jax.numpy as jnp
from jax import lax

K = 16
W = 384
E = 64
NB = 4
FL = 4
ITERS = 2
PD = 8
PATCHES = 64
CELLS = 8


def draw_near_blocks(key, part):
    spread = 0.35 / math.sqrt(W * NB)
    noise = jax.random.normal(key, (PATCHES, NB, W, W), jnp.float32) * spread
    selfpart = (jnp.arange(NB) == 0).astype(jnp.float32)[:, None, None] * jnp.eye(W, dtype=jnp.float32) * 4.0
    return (noise + selfpart[None]).astype(jnp.bfloat16)


def draw_neighbours(key, part):
    labels = jnp.arange(PATCHES, dtype=jnp.int32)
    owner = labels // PD
    offset = jax.random.randint(jax.random.fold_in(key, 11), (PATCHES, NB), 0, 3 * PD, dtype=jnp.int32) - PD
    chosen = jnp.mod(owner[:, None] * PD + offset, PATCHES).astype(jnp.int32)
    return chosen.at[:, 0].set(labels)


def draw_far_lists(key, part):
    labels = jnp.arange(CELLS, dtype=jnp.int32)
    offset = jax.random.randint(jax.random.fold_in(key, 23), (CELLS, FL), 1, CELLS, dtype=jnp.int32)
    side = jax.random.randint(jax.random.fold_in(key, 29), (CELLS,), 0, 2, dtype=jnp.int32) * 2 - 1
    side = jnp.where(labels == 0, -1, side).astype(jnp.int32)
    offset = offset.at[:, 0].set(side)
    return jnp.mod(labels[:, None] + offset, CELLS).astype(jnp.int32)


def level_of(key, dims, cuts, low, high):
    gain, own = 1.0, jax.random.fold_in(key, 6)
    for position, shards_of in cuts:
        steps = jnp.exp(jax.random.uniform(jax.random.fold_in(own, position), (shards_of,), jnp.float32, low / len(cuts), high / len(cuts)))
        gain = gain * jnp.repeat(steps, dims[position] // shards_of).reshape([-1 if axis == position else 1 for axis in range(len(dims))])
    return gain


def normal_values(rng, extent, deviation, bound, split=(), kind=jnp.bfloat16):
    loudness = level_of(rng, extent, split, -0.22, 0.18) if split else 1.0
    drawn = jax.random.normal(rng, extent, jnp.float32) * deviation * loudness
    return jnp.minimum(jnp.maximum(drawn, -bound), bound).astype(kind)


def setup_inputs(seed: int = 0) -> dict:
    seeds = jax.random.split(jax.random.key(seed), 10)
    return {
        "rhs_vectors": normal_values(seeds[0], (PATCHES, K, W), 2.0, 8.0, ((0, 8), (1, 4)), jnp.float32),
        "near_blocks": draw_near_blocks(jax.random.fold_in(seeds[9], 71), 0),
        "neighbours": draw_neighbours(jax.random.fold_in(seeds[9], 71), 0),
        "up_maps": normal_values(seeds[3], (PATCHES, E, W), W ** -0.5, 0.3125, ((0, 8),), jnp.float32),
        "shift_up": normal_values(seeds[4], (PATCHES, E, E), (E * PD) ** -0.5, 0.25, ((0, 8),), jnp.float32),
        "far_lists": draw_far_lists(jax.random.fold_in(seeds[9], 71), 0),
        "translations": normal_values(seeds[6], (CELLS, FL, E, E), (E * FL) ** -0.5, 0.375, ((0, 8),), jnp.float32),
        "shift_down": normal_values(seeds[7], (PATCHES, E, E), E ** -0.5, 0.75, ((0, 8),), jnp.float32),
        "down_maps": normal_values(seeds[8], (PATCHES, W, E), (4 * E) ** -0.5, 0.375, ((0, 8),), jnp.float32),
    }


HIGH = lax.Precision.HIGHEST

def spd_solve(matrix, right):
    factor = jnp.linalg.cholesky(matrix)
    return jax.scipy.linalg.cho_solve((factor, True), right)

def gram(left, right):
    return jnp.einsum('pkw,plw->kl', left, right, precision=HIGH)

def mix(field, coeffs):
    return jnp.einsum('pkw,kl->plw', field, coeffs, precision=HIGH)

def operator(field, near_blocks, neighbours, up_maps, shift_up, far_lists, translations, shift_down, down_maps):
    rounded = lax.optimization_barrier(field.astype(jnp.bfloat16)).astype(jnp.float32)
    picked = rounded[neighbours]
    near = jnp.einsum('pjvw,pjkw->pkv', near_blocks.astype(jnp.float32), picked, precision=HIGH)
    moments = jnp.einsum('pew,pkw->pke', up_maps, field, precision=HIGH)
    cells = moments.reshape(CELLS, PD, K, E)
    shifts = shift_up.reshape(CELLS, PD, E, E)
    cell_moment = jnp.einsum('cpfe,cpke->ckf', shifts, cells, precision=HIGH)
    sources = cell_moment[far_lists]
    local_exp = jnp.einsum('cjfe,cjke->ckf', translations, sources, precision=HIGH)
    spread = jnp.repeat(local_exp, PD, axis=0)
    patch_exp = jnp.einsum('pfe,pke->pkf', shift_down, spread, precision=HIGH)
    far = jnp.einsum('pvf,pkf->pkv', down_maps, patch_exp, precision=HIGH)
    return near + far

def reference(rhs_vectors, near_blocks, neighbours, up_maps, shift_up, far_lists, translations, shift_down, down_maps):
    residual = rhs_vectors
    solution = jnp.zeros_like(residual)
    direction = residual
    current = gram(residual, residual)
    for step in range(ITERS):
        image = operator(direction, near_blocks, neighbours, up_maps, shift_up, far_lists, translations, shift_down, down_maps)
        curve = gram(direction, image)
        curve = 0.5 * (curve + curve.T)
        alpha = spd_solve(curve, current)
        solution = solution + mix(direction, alpha)
        residual = residual - mix(image, alpha)
        if step + 1 < ITERS:
            following = gram(residual, residual)
            beta = spd_solve(current, following)
            direction = residual + mix(direction, beta)
            current = following
    return (solution, residual)
```

```python
import functools

import jax
import jax.numpy as jnp
from jax import lax
from jax.experimental import pallas as pl
from jax.experimental.pallas import tpu as pltpu
from jax.sharding import PartitionSpec as P

MESH = pl.DeviceIdType.MESH
F32 = jnp.float32
BF16 = jnp.bfloat16


def nt(a, b):
    return lax.dot_general(a, b, (((1,), (1,)), ((), ())), preferred_element_type=F32)


def nn(a, b):
    return lax.dot_general(a, b, (((1,), (0,)), ((), ())), preferred_element_type=F32)


def wrap(i, n):
    return jnp.where(i >= n, i - n, i)


def split(x):
    high = x.astype(BF16)
    return high, (x - high.astype(F32)).astype(BF16)


def split3(x):
    high = x.astype(BF16)
    rest = x - high.astype(F32)
    middle = rest.astype(BF16)
    return high, middle, (rest - middle.astype(F32)).astype(BF16)


def rows_of(parts):
    return jnp.concatenate([x.astype(F32) for x in parts], axis=0).astype(BF16)


def exact(form, a, b):
    return lax.dot_general(
        a,
        b,
        (((1,), (0 if form is nn else 1,)), ((), ())),
        precision=lax.Precision.HIGHEST,
        preferred_element_type=F32,
    )


def product(form, a, b):
    ah, al = split(a)
    bh, bl = split(b)
    return form(ah, bh) + (form(ah, bl) + form(al, bh))


def eliminate(systems, n):
    state = [
        (a, [jnp.broadcast_to(a[:, first + j : first + j + 1], a.shape) for j in range(n)])
        for a, first in systems
    ]
    rows = lax.broadcasted_iota(jnp.int32, systems[0][0].shape, 0)
    for k in range(n):
        after = []
        for a, cols in state:
            pivot = cols[k]
            scale = 1.0 / pivot[k : k + 1, :]

            def update(x):
                row = x[k : k + 1, :] * scale
                return jnp.where(rows == k, row, x - pivot * row)

            after.append((update(a), [update(x) if j > k else x for j, x in enumerate(cols)]))
        state = after
    return [a for a, _ in state]


def kernel(
    cells,
    zs,
    chunks,
    rhs_hbm,
    near_hbm,
    neigh,
    up_hbm,
    su_hbm,
    far,
    tr_hbm,
    sd_hbm,
    dn_hbm,
    out,
    rhs,
    blocks,
    up,
    su,
    tr,
    sd,
    dn,
    ucat,
    gcat,
    halo0,
    halo1,
    mom0_out,
    mom0,
    momi_out,
    momi,
    loc_out,
    loc,
    gath_r,
    gath_i,
    base,
    img,
    part_r,
    part_s,
    first,
    second,
    gram_out,
    grams,
    turned,
    near_sem,
    map_sem,
    h0_s,
    h0_r,
    m0_s,
    m0_r,
    gr_s,
    gr_r,
    gi_s,
    gi_r,
    lo_s,
    lo_r,
    g_s,
    g_r,
    mi_s,
    mi_r,
    h1_s,
    h1_r,
):
    c = lax.axis_index("patch")
    z = lax.axis_index("rhs")
    patches, cols, width = rhs.shape
    terms = su.shape[1]
    k = cols * zs
    total = patches * cells
    lists = far.shape[1]
    near_count = neigh.shape[0]

    maps = [(rhs_hbm, rhs), (up_hbm, up), (su_hbm, su), (sd_hbm, sd), (dn_hbm, dn), (tr_hbm, tr)]
    map_copies = [
        pltpu.make_async_copy(src, dst, map_sem.at[i]) for i, (src, dst) in enumerate(maps)
    ]

    def near_copy(p, rest):
        part = pl.ds(1, near_count - 1) if rest else pl.ds(0, 1)
        return pltpu.make_async_copy(
            near_hbm.at[p, part], blocks.at[p, part], near_sem.at[p, 1 if rest else 0]
        )

    for copy in map_copies[:3]:
        copy.start()
    barrier = pltpu.get_barrier_semaphore()

    def cell_of(i):
        return wrap(c + i, cells)

    def row_of(i):
        return wrap(z + i, zs)

    for i in range(1, cells):
        pl.semaphore_signal(barrier, inc=1, device_id=(cell_of(i), z), device_id_type=MESH)
    for i in range(1, zs):
        pl.semaphore_signal(barrier, inc=1, device_id=(c, row_of(i)), device_id_type=MESH)
    for p in range(patches):
        near_copy(p, False).start()
    for copy in map_copies[3:]:
        copy.start()
    for p in range(patches):
        near_copy(p, True).start()

    def send(src, dst, ssem, rsem, device):
        return pltpu.make_async_remote_copy(
            src_ref=src,
            dst_ref=dst,
            send_sem=ssem,
            recv_sem=rsem,
            device_id=device,
            device_id_type=MESH,
        )

    def halo0_copy(side):
        return send(
            halo0.at[pl.ds(patches, patches)],
            halo0.at[pl.ds(0 if side == 0 else 2 * patches, patches)],
            h0_s.at[side],
            h0_r.at[side],
            (cell_of(1 if side == 0 else cells - 1), z),
        )

    step = patches // chunks

    def halo1_copy(side, i):
        return send(
            halo1.at[pl.ds(patches + i * step, step)],
            halo1.at[pl.ds((0 if side == 0 else 2 * patches) + i * step, step)],
            h1_s.at[side, i],
            h1_r.at[side, i],
            (cell_of(1 if side == 0 else cells - 1), z),
        )

    def plane_copy(src, buf, ssem, rsem, target, slot):
        return send(src, buf.at[slot], ssem.at[target], rsem.at[slot], (target, z))

    def z_copy(src, buf, ssem, rsem, target, slot):
        return send(src, buf.at[slot], ssem.at[target], rsem.at[slot], (c, target))

    def image_copy(p, target, slot):
        return send(
            gath_i.at[z, p], gath_i.at[slot, p], gi_s.at[target, p], gi_r.at[slot, p], (c, target)
        )

    def plane(body):
        for i in range(1, cells):
            body(cell_of(i))

    def line(body):
        for i in range(1, zs):
            body(row_of(i))

    def moment0_copy(target, slot):
        return plane_copy(mom0_out, mom0, m0_s, m0_r, target, slot)

    def momenti_copy(target, slot):
        return plane_copy(momi_out, momi, mi_s, mi_r, target, slot)

    def gram_copy(it, target, slot):
        return plane_copy(gram_out.at[it], grams.at[it], g_s.at[it], g_r.at[it], target, slot)

    def rhs_copy(target, slot):
        return z_copy(rhs, gath_r, gr_s, gr_r, target, slot)

    def local_copy(target, slot):
        return z_copy(loc_out, loc, lo_s, lo_r, target, slot)

    map_copies[0].wait()
    for p in range(patches):
        halo0[patches + p] = rhs[p].astype(BF16)
    pl.semaphore_wait(barrier, cells - 1 + zs - 1)
    halo0_copy(0).start()
    halo0_copy(1).start()
    line(lambda t: rhs_copy(t, z).start())

    map_copies[1].wait()
    map_copies[2].wait()
    acc = jnp.zeros((2 * cols, 2 * terms), F32)
    for p in range(patches):
        high, low = split(product(nn, su[p], up[p]))
        ucat[p, 0:terms, :] = high
        ucat[p, terms : 2 * terms, :] = low
        acc = acc + nt(rows_of(split(rhs[p])), ucat[p])
    acc = acc[0:cols] + acc[cols:]
    mom0_out[...] = jnp.concatenate([acc[:, 0:terms] + acc[:, terms:], jnp.zeros_like(acc[:, terms:])], axis=1)
    mom0[c] = mom0_out[...]
    plane(lambda t: moment0_copy(t, c).start())

    for p in range(patches):
        near_copy(p, False).wait()
        gath_i[z, p] = nt(halo0[patches + p], blocks[p, 0])
    for p in range(patches):
        gath_r[z, p] = rhs[p]

    for copy in map_copies[3:]:
        copy.wait()
    for p in range(patches):
        high, low = split(product(nn, sd[p].T, dn[p]))
        gcat[p, 0:terms, :] = high
        gcat[p, terms : 2 * terms, :] = low
    tall = jnp.concatenate([tr[0, j] for j in range(lists)], axis=1)

    def spot_of(p, j):
        spot = wrap(neigh[j, p] - (c * patches - patches) + total, total)
        return jnp.minimum(wrap(spot, total), 3 * patches - 1)

    halo0_copy(0).wait_recv()
    halo0_copy(1).wait_recv()
    for p in range(patches):
        near_copy(p, True).wait()
        acc = gath_i[z, p]
        for j in range(1, near_count):
            acc = acc + nt(halo0[spot_of(p, j)], blocks[p, j])
        gath_i[z, p] = acc
        line(lambda t, p=p: image_copy(p, t, z).start())

    def local_of(moments):
        wide = jnp.concatenate([moments[far[0, j]][:, 0:terms] for j in range(lists)], axis=1)
        return product(nt, wide, tall)

    plane(lambda s: moment0_copy(s, s).wait_recv())
    loc_out[...] = jnp.zeros(loc_out.shape, F32)
    loc_out[:, 0:terms] = local_of(mom0)
    loc[z] = loc_out[...]
    line(lambda t: local_copy(t, z).start())

    def far_of(local, p):
        high, low = split(local)
        both = jnp.concatenate(
            [jnp.concatenate([high, high], axis=1), jnp.concatenate([low, low], axis=1)], axis=0
        )
        both = nn(both, gcat[p])
        return both[0:k] + both[k:]

    line(lambda s: rhs_copy(s, s).wait_recv())
    for p in range(patches):
        for s in range(zs):
            img[p, s * cols : (s + 1) * cols, :] = gath_r[s, p]
        for i, x in enumerate(split3(img[p])):
            first[p, 2 * i * k : (2 * i + 1) * k, :] = x

    line(lambda s: local_copy(s, s).wait_recv())
    for s in range(zs):
        base[s * cols : (s + 1) * cols, :] = loc[s]
    local0 = base[:, 0:terms]
    acc1 = jnp.zeros((4 * k, 2 * k), F32)
    acc2 = jnp.zeros((4 * k, 2 * k), F32)
    for p in range(patches):
        whole = far_of(local0, p)
        line(lambda s, p=p: image_copy(p, s, s).wait_recv())
        for s in range(zs):
            img[p, s * cols : (s + 1) * cols, :] = gath_i[s, p]
        for i, x in enumerate(split3(img[p] + whole)):
            first[p, (2 * i + 1) * k : (2 * i + 2) * k, :] = x
        acc1 = acc1 + nt(first[p, 0 : 4 * k], first[p, 0 : 2 * k])
        acc2 = acc2 + nt(first[p, 0 : 4 * k], first[p, 2 * k : 4 * k])
    gram = acc1[0 : 2 * k] + (acc1[2 * k :] + acc2[0 : 2 * k] + acc2[2 * k :])
    top, low = gram[0:k], gram[k:]
    gram_out[0] = jnp.concatenate(
        [
            0.5 * (top[:, k:] + low[:, 0:k]),
            top[:, 0:k],
            low,
            top,
            jnp.zeros((k, 128 - 6 * k), F32),
        ],
        axis=1,
    )
    grams[0, c] = gram_out[0]
    plane(lambda t: gram_copy(0, t, c).start())

    acc = jnp.zeros((2 * k, 2 * terms), F32)
    for p in range(patches):
        acc = acc + nt(
            jnp.concatenate([first[p, k : 2 * k], first[p, 3 * k : 4 * k]], axis=0), ucat[p]
        )
    acc = acc[0:k] + acc[k:]
    momi_out[...] = jnp.concatenate([acc[:, 0:terms] + acc[:, terms:], jnp.zeros_like(acc[:, terms:])], axis=1)
    momi[c] = momi_out[...]
    plane(lambda t: momenti_copy(t, c).start())

    def collect(it):
        plane(lambda s: gram_copy(it, s, s).wait_recv())
        parts = [grams[it, i] for i in range(cells)]
        while len(parts) > 1:
            parts = [
                parts[i] + parts[i + 1] if i + 1 < len(parts) else parts[i]
                for i in range(0, len(parts), 2)
            ]
        return parts[0]

    eye = (
        lax.broadcasted_iota(jnp.int32, (k, k), 1) == lax.broadcasted_iota(jnp.int32, (k, k), 0)
    ).astype(F32)
    got = collect(0)
    one, two = eliminate([(got, 0), (got, 4 * k)], k)
    one_t, two_t = one.T, two.T
    alpha_t = one_t[k : 2 * k]
    beta1_t = (
        2.0 * eye
        - one_t[2 * k : 3 * k]
        + exact(nn, alpha_t, one_t[3 * k : 4 * k] - two_t[5 * k : 6 * k])
    )

    def doubled(x):
        high, low = split(x)
        high, low = high.astype(F32), low.astype(F32)
        return jnp.concatenate(
            [jnp.concatenate([high, high], axis=1), jnp.concatenate([low, low], axis=1)], axis=0
        ).astype(BF16)

    mixing = jnp.concatenate(
        [
            jnp.concatenate([x.astype(F32)] * 3, axis=1)
            for x in split3(jnp.concatenate([beta1_t, -alpha_t], axis=1))
        ],
        axis=0,
    ).astype(BF16)
    for p in range(patches):
        both = nn(mixing, first[p])
        high, low = split(both[0:k] + (both[k : 2 * k] + both[2 * k :]))
        halo1[patches + p] = high
        second[p, 0:k, :] = high
        second[p, k : 2 * k, :] = low
        if (p + 1) % step == 0:
            halo1_copy(0, p // step).start()
            halo1_copy(1, p // step).start()

    plane(lambda s: momenti_copy(s, s).wait_recv())
    local1 = product(nn, beta1_t, local0) - product(nn, alpha_t, local_of(momi))
    for p in range(patches):
        img[p] = nt(halo1[patches + p], blocks[p, 0]) + far_of(local1, p)
    mixed = exact(nt, got[:, 5 * k : 6 * k], alpha_t)
    new = (
        got[:, k : 2 * k]
        - mixed
        - mixed.T
        + exact(nn, alpha_t, exact(nt, got[:, 3 * k : 4 * k], alpha_t))
    )
    base[...] = jnp.zeros(base.shape, F32)
    base[:, k : 2 * k] = new
    right = base[...]
    turned[...] = one_t
    own = turned[pl.ds(k + z * cols, cols), :]
    high, low = [x.astype(F32) for x in split(own)]
    none = jnp.zeros_like(own)
    out_mix = jnp.concatenate(
        [
            jnp.concatenate([high, none, high, none], axis=1),
            jnp.concatenate([low, none, low, none], axis=1),
            jnp.concatenate([none, high, none, high], axis=1),
            jnp.concatenate([none, low, none, low], axis=1),
        ],
        axis=0,
    ).astype(BF16)
    for p in range(patches):
        both = nn(out_mix, first[p, 0 : 4 * k])
        part_s[p] = both[0:cols] + both[cols : 2 * cols]
        part_r[p] = rhs[p] - (both[2 * cols : 3 * cols] + both[3 * cols :])

    for i in range(chunks):
        halo1_copy(0, i).wait_recv()
        halo1_copy(1, i).wait_recv()
    acc1 = jnp.zeros((2 * k, k), F32)
    acc2 = jnp.zeros((k, k), F32)
    for p in range(patches):
        acc = img[p]
        for j in range(1, near_count):
            acc = acc + nt(halo1[spot_of(p, j)], blocks[p, j])
        high, low = split(acc)
        second[p, 2 * k : 3 * k, :] = high
        second[p, 3 * k : 4 * k, :] = low
        acc1 = acc1 + nt(second[p, 0 : 2 * k], high)
        acc2 = acc2 + nt(second[p, 0:k], low)
    curve = acc1[0:k] + acc1[k:] + acc2
    gram_out[1] = jnp.concatenate(
        [0.5 * (curve + curve.T), jnp.zeros((k, 128 - k), F32)], axis=1
    )
    grams[1, c] = gram_out[1]
    plane(lambda t: gram_copy(1, t, c).start())
    (last,) = eliminate([(collect(1) + right, 0)], k)
    turned[...] = last.T
    out_mix = doubled(turned[pl.ds(k + z * cols, cols), :])
    for p in range(patches):
        both = nn(out_mix, second[p, 0 : 2 * k])
        out[p, 0:cols, :] = part_s[p] + (both[0:cols] + both[cols:])
        both = nn(out_mix, second[p, 2 * k : 4 * k])
        out[p, cols : 2 * cols, :] = part_r[p] - (both[0:cols] + both[cols:])

    for side in range(2):
        halo0_copy(side).wait_send()
        for i in range(chunks):
            halo1_copy(side, i).wait_send()
    line(lambda t: rhs_copy(t, z).wait_send())
    line(lambda t: local_copy(t, z).wait_send())
    for p in range(patches):
        line(lambda t, p=p: image_copy(p, t, z).wait_send())
    plane(lambda t: moment0_copy(t, c).wait_send())
    plane(lambda t: momenti_copy(t, c).wait_send())
    for it in range(2):
        plane(lambda t, it=it: gram_copy(it, t, c).wait_send())


def on_device(cells, zs, *args):
    rhs, near, neigh, up, su, far, tr, sd, dn = args
    patches, cols, width = rhs.shape
    terms = su.shape[1]
    dn = jnp.swapaxes(dn, 1, 2)
    neigh = neigh.T
    k = cols * zs
    chunks = 4 if patches % 4 == 0 else 1
    vmem = pl.BlockSpec(memory_space=pltpu.VMEM)
    smem = pl.BlockSpec(memory_space=pltpu.SMEM)
    hbm = pl.BlockSpec(memory_space=pltpu.HBM)
    dma = pltpu.SemaphoreType.DMA
    out = pl.pallas_call(
        functools.partial(kernel, cells, zs, chunks),
        out_shape=jax.ShapeDtypeStruct((patches, 2 * cols, width), F32),
        in_specs=[hbm, hbm, smem, hbm, hbm, smem, hbm, hbm, hbm],
        out_specs=vmem,
        scratch_shapes=[
            pltpu.VMEM(rhs.shape, F32),
            pltpu.VMEM(near.shape, near.dtype),
            pltpu.VMEM(up.shape, F32),
            pltpu.VMEM(su.shape, F32),
            pltpu.VMEM(tr.shape, F32),
            pltpu.VMEM(sd.shape, F32),
            pltpu.VMEM(dn.shape, F32),
            pltpu.VMEM((patches, 2 * terms, width), BF16),
            pltpu.VMEM((patches, 2 * terms, width), BF16),
            pltpu.VMEM((3 * patches, cols, width), BF16),
            pltpu.VMEM((3 * patches, k, width), BF16),
            pltpu.VMEM((cols, 128), F32),
            pltpu.VMEM((cells, cols, 128), F32),
            pltpu.VMEM((k, 128), F32),
            pltpu.VMEM((cells, k, 128), F32),
            pltpu.VMEM((cols, 128), F32),
            pltpu.VMEM((zs, cols, 128), F32),
            pltpu.VMEM((zs,) + rhs.shape, F32),
            pltpu.VMEM((zs,) + rhs.shape, F32),
            pltpu.VMEM((k, 128), F32),
            pltpu.VMEM((patches, k, width), F32),
            pltpu.VMEM(rhs.shape, F32),
            pltpu.VMEM(rhs.shape, F32),
            pltpu.VMEM((patches, 6 * k, width), BF16),
            pltpu.VMEM((patches, 4 * k, width), BF16),
            pltpu.VMEM((2, k, 128), F32),
            pltpu.VMEM((2, cells, k, 128), F32),
            pltpu.VMEM((128, k), F32),
            dma((patches, 2)),
            dma((6,)),
            dma((2,)),
            dma((2,)),
            dma((cells,)),
            dma((cells,)),
            dma((zs,)),
            dma((zs,)),
            dma((zs, patches)),
            dma((zs, patches)),
            dma((zs,)),
            dma((zs,)),
            dma((2, cells)),
            dma((2, cells)),
            dma((cells,)),
            dma((cells,)),
            dma((2, chunks)),
            dma((2, chunks)),
        ],
        compiler_params=pltpu.CompilerParams(
            collective_id=0, has_side_effects=True, vmem_limit_bytes=60 * 1024 * 1024
        ),
        name="block_cg",
    )(rhs, near, neigh, up, su, far, tr, sd, dn)
    return out[:, 0:cols], out[:, cols:]


def solution(mesh):
    cells = mesh.shape["patch"]
    zs = mesh.shape["rhs"]
    return jax.shard_map(
        functools.partial(on_device, cells, zs),
        mesh=mesh,
        in_specs=(
            P("patch", "rhs", None),
            P("patch", None, None, None),
            P("patch", None),
            P("patch", None, None),
            P("patch", None, None),
            P("patch", None),
            P("patch", None, None, None),
            P("patch", None, None),
            P("patch", None, None),
        ),
        out_specs=(P("patch", "rhs", None), P("patch", "rhs", None)),
        check_vma=False,
    )
```

```python
import functools

import jax
import jax.numpy as jnp
from jax import lax
from jax.experimental import pallas as pl
from jax.experimental.pallas import tpu as pltpu
from jax.sharding import PartitionSpec as P

MESH = pl.DeviceIdType.MESH
F32 = jnp.float32
BF16 = jnp.bfloat16


def nt(a, b):
    return lax.dot_general(a, b, (((1,), (1,)), ((), ())), preferred_element_type=F32)


def nn(a, b):
    return lax.dot_general(a, b, (((1,), (0,)), ((), ())), preferred_element_type=F32)


def wrap(i, n):
    return jnp.where(i >= n, i - n, i)


def split(x):
    high = x.astype(BF16)
    return high, (x - high.astype(F32)).astype(BF16)


def split3(x):
    high = x.astype(BF16)
    rest = x - high.astype(F32)
    middle = rest.astype(BF16)
    return high, middle, (rest - middle.astype(F32)).astype(BF16)


def rows_of(parts):
    return jnp.concatenate([x.astype(F32) for x in parts], axis=0).astype(BF16)


def exact(form, a, b):
    return lax.dot_general(
        a,
        b,
        (((1,), (0 if form is nn else 1,)), ((), ())),
        precision=lax.Precision.HIGHEST,
        preferred_element_type=F32,
    )


def product(form, a, b):
    ah, al = split(a)
    bh, bl = split(b)
    return form(ah, bh) + (form(ah, bl) + form(al, bh))


def eliminate(systems, n):
    state = [
        (a, [jnp.broadcast_to(a[:, first + j : first + j + 1], a.shape) for j in range(n)])
        for a, first in systems
    ]
    rows = lax.broadcasted_iota(jnp.int32, systems[0][0].shape, 0)
    for k in range(n):
        after = []
        for a, cols in state:
            pivot = cols[k]
            scale = 1.0 / pivot[k : k + 1, :]

            def update(x):
                row = x[k : k + 1, :] * scale
                return jnp.where(rows == k, row, x - pivot * row)

            after.append((update(a), [update(x) if j > k else x for j, x in enumerate(cols)]))
        state = after
    return [a for a, _ in state]


def kernel(
    cells,
    zs,
    chunks,
    rhs_hbm,
    near_hbm,
    neigh,
    up_hbm,
    su_hbm,
    far,
    tr_hbm,
    sd_hbm,
    dn_hbm,
    out,
    rhs,
    blocks,
    up,
    su,
    tr,
    sd,
    dn,
    ucat,
    gcat,
    halo0,
    halo1,
    mom0_out,
    mom0,
    momi_out,
    momi,
    loc_out,
    loc,
    gath_r,
    gath_i,
    base,
    img,
    part_r,
    part_s,
    first,
    second,
    gram_out,
    grams,
    turned,
    near_sem,
    map_sem,
    h0_s,
    h0_r,
    m0_s,
    m0_r,
    gr_s,
    gr_r,
    gi_s,
    gi_r,
    lo_s,
    lo_r,
    g_s,
    g_r,
    mi_s,
    mi_r,
    h1_s,
    h1_r,
    in_above,
    in_below,
):
    c = lax.axis_index("patch")
    z = lax.axis_index("rhs")
    patches, cols, width = rhs.shape
    terms = su.shape[1]
    k = cols * zs
    total = patches * cells
    lists = far.shape[1]
    near_count = neigh.shape[0]

    maps = [(rhs_hbm, rhs), (up_hbm, up), (su_hbm, su), (sd_hbm, sd), (dn_hbm, dn), (tr_hbm, tr)]
    map_copies = [
        pltpu.make_async_copy(src, dst, map_sem.at[i]) for i, (src, dst) in enumerate(maps)
    ]

    def near_copy(p, rest):
        part = pl.ds(1, near_count - 1) if rest else pl.ds(0, 1)
        return pltpu.make_async_copy(
            near_hbm.at[p, part], blocks.at[p, part], near_sem.at[p, 1 if rest else 0]
        )

    for copy in map_copies[:3]:
        copy.start()
    barrier = pltpu.get_barrier_semaphore()

    def cell_of(i):
        return wrap(c + i, cells)

    def row_of(i):
        return wrap(z + i, zs)

    for i in range(1, cells):
        pl.semaphore_signal(barrier, inc=1, device_id=(cell_of(i), z), device_id_type=MESH)

    def below(i, body):
        pl.when(z >= i)(body)

    def above(i, body):
        pl.when(z < zs - i)(body)

    below(1, lambda: pl.semaphore_signal(barrier, inc=1, device_id=(c, z - 1), device_id_type=MESH))
    above(1, lambda: pl.semaphore_signal(barrier, inc=1, device_id=(c, z + 1), device_id_type=MESH))

    def tell(i):
        def down():
            pl.semaphore_signal(in_above.at[i - 1], inc=1, device_id=(c, z - 1), device_id_type=MESH)

        def up():
            pl.semaphore_signal(in_below.at[i - 1], inc=1, device_id=(c, z + 1), device_id_type=MESH)

        pl.when((z >= 1) & (z < zs - i))(down)
        pl.when((z >= i) & (z < zs - 1))(up)

    def hear(i):
        above(i + 1, lambda: pl.semaphore_wait(in_above.at[i - 1], 1))
        below(i + 1, lambda: pl.semaphore_wait(in_below.at[i - 1], 1))


    def send(src, dst, ssem, rsem, device):
        return pltpu.make_async_remote_copy(
            src_ref=src,
            dst_ref=dst,
            send_sem=ssem,
            recv_sem=rsem,
            device_id=device,
            device_id_type=MESH,
        )

    def halo0_copy(side):
        return send(
            halo0.at[pl.ds(patches, patches)],
            halo0.at[pl.ds(0 if side == 0 else 2 * patches, patches)],
            h0_s.at[side],
            h0_r.at[side],
            (cell_of(1 if side == 0 else cells - 1), z),
        )

    step = patches // chunks

    def halo1_copy(side, i):
        return send(
            halo1.at[pl.ds(patches + i * step, step)],
            halo1.at[pl.ds((0 if side == 0 else 2 * patches) + i * step, step)],
            h1_s.at[side, i],
            h1_r.at[side, i],
            (cell_of(1 if side == 0 else cells - 1), z),
        )

    def plane_copy(src, buf, ssem, rsem, target, slot):
        return send(src, buf.at[slot], ssem.at[target], rsem.at[slot], (target, z))

    def z_copy(src, buf, ssem, rsem, target, slot):
        return send(src, buf.at[slot], ssem.at[target], rsem.at[slot], (c, target))

    pieces = 4 if patches % 4 == 0 else 1
    piece = patches // pieces
    group = 2 if pieces > 1 else 1

    def image_copy(i, target, slot):
        part = pl.ds(i * piece, piece)
        return send(
            gath_i.at[z, part],
            gath_i.at[slot, part],
            gi_s.at[target, i],
            gi_r.at[slot, i],
            (c, target),
        )

    def plane(body):
        for i in range(1, cells):
            body(cell_of(i))

    def line(body):
        for i in range(1, zs):
            body(row_of(i))

    def moment0_copy(target, slot):
        return plane_copy(mom0_out, mom0, m0_s, m0_r, target, slot)

    def momenti_copy(target, slot):
        return plane_copy(momi_out, momi, mi_s, mi_r, target, slot)

    def gram_copy(it, target, slot):
        return plane_copy(gram_out.at[it], grams.at[it], g_s.at[it], g_r.at[it], target, slot)

    def rhs_copy(target, slot):
        return z_copy(rhs, gath_r, gr_s, gr_r, target, slot)

    def local_copy(target, slot):
        return z_copy(loc_out, loc, lo_s, lo_r, target, slot)

    map_copies[0].wait()
    for p in range(patches):
        near_copy(p, False).start()
    for p in range(patches):
        near_copy(p, True).start()
    for copy in map_copies[3:]:
        copy.start()
    for p in range(patches):
        halo0[patches + p] = rhs[p].astype(BF16)
        gath_r[z, p] = rhs[p]
    map_copies[1].wait()
    map_copies[2].wait()

    pl.semaphore_wait(barrier, cells - 1 + jnp.where(z > 0, 1, 0) + jnp.where(z < zs - 1, 1, 0))
    halo0_copy(0).start()
    halo0_copy(1).start()

    def share(i):
        below(i, lambda: rhs_copy(z - i, z).start())
        above(i, lambda: rhs_copy(z + i, z).start())

    if zs > 2:
        tell(1)
    share(1)

    acc = jnp.zeros((2 * cols, 2 * terms), F32)
    for p in range(patches):
        high, low = split(product(nn, su[p], up[p]))
        ucat[p, 0:terms, :] = high
        ucat[p, terms : 2 * terms, :] = low
        acc = acc + nt(rows_of(split(rhs[p])), ucat[p])
    acc = acc[0:cols] + acc[cols:]
    acc = acc[:, 0:terms] + acc[:, terms:]
    mom0_out[...] = jnp.concatenate([acc, jnp.zeros((cols, 128 - terms), F32)], axis=1)
    mom0[c] = mom0_out[...]
    plane(lambda t: moment0_copy(t, c).start())
    if zs > 2:
        hear(1)
        if zs > 3:
            tell(2)
        share(2)

    for p in range(patches):
        near_copy(p, False).wait()
    for p in range(patches):
        gath_i[z, p] = nt(halo0[patches + p], blocks[p, 0])
    for i in range(2, zs - 1):
        hear(i)
        if i < zs - 2:
            tell(i + 1)
        share(i + 1)

    map_copies[5].wait()
    tall = jnp.concatenate([tr[0, j] for j in range(lists)], axis=1)

    def spot_of(p, j):
        spot = wrap(neigh[j, p] - (c * patches - patches) + total, total)
        return jnp.minimum(wrap(spot, total), 3 * patches - 1)

    def local_of(moments):
        wide = jnp.concatenate([moments[far[0, j]][:, 0:terms] for j in range(lists)], axis=1)
        return product(nt, wide, tall)

    for p in range(patches):
        near_copy(p, True).wait()
    halo0_copy(0).wait_recv()
    halo0_copy(1).wait_recv()
    for i in range(pieces):
        for p in range(i * piece, (i + 1) * piece):
            acc = gath_i[z, p]
            for j in range(1, near_count):
                acc = acc + nt(halo0[spot_of(p, j)], blocks[p, j])
            gath_i[z, p] = acc
        line(lambda t, i=i: image_copy(i, t, z).start())
        if i == pieces // 2 - 1 or pieces == 1:
            plane(lambda s: moment0_copy(s, s).wait_recv())
            loc_out[...] = jnp.concatenate(
                [local_of(mom0), jnp.zeros((cols, 128 - terms), F32)], axis=1
            )
            loc[z] = loc_out[...]
            line(lambda t: local_copy(t, z).start())

    def far_of(local, p):
        high, low = split(local)
        both = jnp.concatenate(
            [jnp.concatenate([high, high], axis=1), jnp.concatenate([low, low], axis=1)], axis=0
        )
        both = nn(both, gcat[p])
        return both[0:k] + both[k:]

    for copy in map_copies[3:5]:
        copy.wait()
    for p in range(patches):
        high, low = split(product(nn, sd[p].T, dn[p]))
        gcat[p, 0:terms, :] = high
        gcat[p, terms : 2 * terms, :] = low

    line(lambda s: rhs_copy(s, s).wait_recv())
    for p in range(patches):
        for i, x in enumerate(split3(jnp.concatenate([gath_r[s, p] for s in range(zs)], axis=0))):
            first[p, 2 * i * k : (2 * i + 1) * k, :] = x

    line(lambda s: local_copy(s, s).wait_recv())
    local0 = jnp.concatenate([loc[s] for s in range(zs)], axis=0)[:, 0:terms]
    for p in range(patches):
        img[p] = far_of(local0, p)
    acc1 = jnp.zeros((4 * k, 2 * k), F32)
    acc2 = jnp.zeros((4 * k, 2 * k), F32)
    for i in range(pieces):
        if i % group == 0:
            for j in range(i, i + group):
                line(lambda s, j=j: image_copy(j, s, s).wait_recv())
        for p in range(i * piece, (i + 1) * piece):
            whole = jnp.concatenate([gath_i[s, p] for s in range(zs)], axis=0) + img[p]
            high, middle, low = split3(whole)
            first[p, k : 2 * k, :] = high
            first[p, 3 * k : 4 * k, :] = middle
            first[p, 5 * k : 6 * k, :] = low
            one = jnp.concatenate([first[p, 0:k], high], axis=0)
            two = jnp.concatenate([first[p, 2 * k : 3 * k], middle], axis=0)
            both = jnp.concatenate([one, two], axis=0)
            acc1 = acc1 + nt(both, one)
            acc2 = acc2 + nt(both, two)
    gram = acc1[0 : 2 * k] + (acc1[2 * k :] + acc2[0 : 2 * k] + acc2[2 * k :])
    top, low = gram[0:k], gram[k:]
    gram_out[0] = jnp.concatenate(
        [
            0.5 * (top[:, k:] + low[:, 0:k]),
            top[:, 0:k],
            low,
            top,
            jnp.zeros((k, 128 - 6 * k), F32),
        ],
        axis=1,
    )
    grams[0, c] = gram_out[0]
    plane(lambda t: gram_copy(0, t, c).start())

    acc = jnp.zeros((2 * k, 2 * terms), F32)
    for p in range(patches):
        acc = acc + nt(
            jnp.concatenate([first[p, k : 2 * k], first[p, 3 * k : 4 * k]], axis=0), ucat[p]
        )
    acc = acc[0:k] + acc[k:]
    acc = acc[:, 0:terms] + acc[:, terms:]
    momi_out[...] = jnp.concatenate([acc, jnp.zeros((k, 128 - terms), F32)], axis=1)
    momi[c] = momi_out[...]
    plane(lambda t: momenti_copy(t, c).start())

    def collect(it):
        plane(lambda s: gram_copy(it, s, s).wait_recv())
        parts = [grams[it, i] for i in range(cells)]
        while len(parts) > 1:
            parts = [
                parts[i] + parts[i + 1] if i + 1 < len(parts) else parts[i]
                for i in range(0, len(parts), 2)
            ]
        return parts[0]

    eye = (
        lax.broadcasted_iota(jnp.int32, (k, k), 1) == lax.broadcasted_iota(jnp.int32, (k, k), 0)
    ).astype(F32)
    got = collect(0)
    one, two = eliminate([(got, 0), (got, 4 * k)], k)
    one_t, two_t = one.T, two.T
    alpha_t = one_t[k : 2 * k]
    beta1_t = (
        2.0 * eye
        - one_t[2 * k : 3 * k]
        + exact(nn, alpha_t, one_t[3 * k : 4 * k] - two_t[5 * k : 6 * k])
    )

    def doubled(x):
        high, low = split(x)
        high, low = high.astype(F32), low.astype(F32)
        return jnp.concatenate(
            [jnp.concatenate([high, high], axis=1), jnp.concatenate([low, low], axis=1)], axis=0
        ).astype(BF16)

    mixing = jnp.concatenate(
        [
            jnp.concatenate([x.astype(F32)] * 3, axis=1)
            for x in split3(jnp.concatenate([beta1_t, -alpha_t], axis=1))
        ],
        axis=0,
    ).astype(BF16)
    for p in range(patches):
        both = nn(mixing, first[p])
        high, low = split(both[0:k] + (both[k : 2 * k] + both[2 * k :]))
        halo1[patches + p] = high
        second[p, 0:k, :] = high
        second[p, k : 2 * k, :] = low
        if (p + 1) % step == 0:
            halo1_copy(0, p // step).start()
            halo1_copy(1, p // step).start()

    plane(lambda s: momenti_copy(s, s).wait_recv())
    local1 = product(nn, beta1_t, local0) - product(nn, alpha_t, local_of(momi))
    for p in range(patches):
        img[p] = nt(halo1[patches + p], blocks[p, 0]) + far_of(local1, p)
    mixed = exact(nt, got[:, 5 * k : 6 * k], alpha_t)
    new = (
        got[:, k : 2 * k]
        - mixed
        - mixed.T
        + exact(nn, alpha_t, exact(nt, got[:, 3 * k : 4 * k], alpha_t))
    )
    base[...] = jnp.zeros(base.shape, F32)
    base[:, k : 2 * k] = new
    right = base[...]
    turned[...] = one_t
    own = turned[pl.ds(k + z * cols, cols), :]
    high, low = [x.astype(F32) for x in split(own)]
    none = jnp.zeros_like(own)
    out_mix = jnp.concatenate(
        [
            jnp.concatenate([high, none, high, none], axis=1),
            jnp.concatenate([low, none, low, none], axis=1),
            jnp.concatenate([none, high, none, high], axis=1),
            jnp.concatenate([none, low, none, low], axis=1),
        ],
        axis=0,
    ).astype(BF16)
    for p in range(patches):
        both = nn(out_mix, first[p, 0 : 4 * k])
        part_s[p] = both[0:cols] + both[cols : 2 * cols]
        part_r[p] = rhs[p] - (both[2 * cols : 3 * cols] + both[3 * cols :])

    for i in range(chunks):
        halo1_copy(0, i).wait_recv()
        halo1_copy(1, i).wait_recv()
    acc1 = jnp.zeros((2 * k, k), F32)
    acc2 = jnp.zeros((k, k), F32)
    for p in range(patches):
        acc = img[p]
        for j in range(1, near_count):
            acc = acc + nt(halo1[spot_of(p, j)], blocks[p, j])
        high, low = split(acc)
        second[p, 2 * k : 3 * k, :] = high
        second[p, 3 * k : 4 * k, :] = low
        acc1 = acc1 + nt(second[p, 0 : 2 * k], high)
        acc2 = acc2 + nt(second[p, 0:k], low)
    curve = acc1[0:k] + acc1[k:] + acc2
    gram_out[1] = jnp.concatenate(
        [0.5 * (curve + curve.T), jnp.zeros((k, 128 - k), F32)], axis=1
    )
    grams[1, c] = gram_out[1]
    plane(lambda t: gram_copy(1, t, c).start())
    (last,) = eliminate([(collect(1) + right, 0)], k)
    turned[...] = last.T
    out_mix = doubled(turned[pl.ds(k + z * cols, cols), :])
    for p in range(patches):
        both = nn(out_mix, second[p, 0 : 2 * k])
        out[p, 0:cols, :] = part_s[p] + (both[0:cols] + both[cols:])
        both = nn(out_mix, second[p, 2 * k : 4 * k])
        out[p, cols : 2 * cols, :] = part_r[p] - (both[0:cols] + both[cols:])

    for side in range(2):
        halo0_copy(side).wait_send()
        for i in range(chunks):
            halo1_copy(side, i).wait_send()
    line(lambda t: rhs_copy(t, z).wait_send())
    line(lambda t: local_copy(t, z).wait_send())
    for i in range(pieces):
        line(lambda t, i=i: image_copy(i, t, z).wait_send())
    plane(lambda t: moment0_copy(t, c).wait_send())
    plane(lambda t: momenti_copy(t, c).wait_send())
    for it in range(2):
        plane(lambda t, it=it: gram_copy(it, t, c).wait_send())


def on_device(cells, zs, *args):
    rhs, near, neigh, up, su, far, tr, sd, dn = args
    patches, cols, width = rhs.shape
    terms = su.shape[1]
    dn = jnp.swapaxes(dn, 1, 2)
    neigh = neigh.T
    k = cols * zs
    chunks = 4 if patches % 4 == 0 else 1
    vmem = pl.BlockSpec(memory_space=pltpu.VMEM)
    smem = pl.BlockSpec(memory_space=pltpu.SMEM)
    hbm = pl.BlockSpec(memory_space=pltpu.HBM)
    dma = pltpu.SemaphoreType.DMA
    out = pl.pallas_call(
        functools.partial(kernel, cells, zs, chunks),
        out_shape=pltpu.VMEM((patches, 2 * cols, width), F32),
        in_specs=[hbm, hbm, smem, hbm, hbm, smem, hbm, hbm, hbm],
        out_specs=vmem,
        scratch_shapes=[
            pltpu.VMEM(rhs.shape, F32),
            pltpu.VMEM(near.shape, near.dtype),
            pltpu.VMEM(up.shape, F32),
            pltpu.VMEM(su.shape, F32),
            pltpu.VMEM(tr.shape, F32),
            pltpu.VMEM(sd.shape, F32),
            pltpu.VMEM(dn.shape, F32),
            pltpu.VMEM((patches, 2 * terms, width), BF16),
            pltpu.VMEM((patches, 2 * terms, width), BF16),
            pltpu.VMEM((3 * patches, cols, width), BF16),
            pltpu.VMEM((3 * patches, k, width), BF16),
            pltpu.VMEM((cols, 128), F32),
            pltpu.VMEM((cells, cols, 128), F32),
            pltpu.VMEM((k, 128), F32),
            pltpu.VMEM((cells, k, 128), F32),
            pltpu.VMEM((cols, 128), F32),
            pltpu.VMEM((zs, cols, 128), F32),
            pltpu.VMEM((zs,) + rhs.shape, F32),
            pltpu.VMEM((zs,) + rhs.shape, F32),
            pltpu.VMEM((k, 128), F32),
            pltpu.VMEM((patches, k, width), F32),
            pltpu.VMEM(rhs.shape, F32),
            pltpu.VMEM(rhs.shape, F32),
            pltpu.VMEM((patches, 6 * k, width), BF16),
            pltpu.VMEM((patches, 4 * k, width), BF16),
            pltpu.VMEM((2, k, 128), F32),
            pltpu.VMEM((2, cells, k, 128), F32),
            pltpu.VMEM((128, k), F32),
            dma((patches, 2)),
            dma((6,)),
            dma((2,)),
            dma((2,)),
            dma((cells,)),
            dma((cells,)),
            dma((zs,)),
            dma((zs,)),
            dma((zs, patches)),
            dma((zs, patches)),
            dma((zs,)),
            dma((zs,)),
            dma((2, cells)),
            dma((2, cells)),
            dma((cells,)),
            dma((cells,)),
            dma((2, chunks)),
            dma((2, chunks)),
            pltpu.SemaphoreType.REGULAR((zs,)),
            pltpu.SemaphoreType.REGULAR((zs,)),
        ],
        compiler_params=pltpu.CompilerParams(
            collective_id=0, has_side_effects=True, vmem_limit_bytes=60 * 1024 * 1024
        ),
        name="block_cg",
    )(rhs, near, neigh, up, su, far, tr, sd, dn)
    return out[:, 0:cols], out[:, cols:]


def solution(mesh):
    cells = mesh.shape["patch"]
    zs = mesh.shape["rhs"]
    return jax.shard_map(
        functools.partial(on_device, cells, zs),
        mesh=mesh,
        in_specs=(
            P("patch", "rhs", None),
            P("patch", None, None, None),
            P("patch", None),
            P("patch", None, None),
            P("patch", None, None),
            P("patch", None),
            P("patch", None, None, None),
            P("patch", None, None),
            P("patch", None, None),
        ),
        out_specs=(P("patch", "rhs", None), P("patch", "rhs", None)),
        check_vma=False,
    )
```

```python
import functools

import jax
import jax.numpy as jnp
from jax import lax
from jax.experimental import pallas as pl
from jax.experimental.pallas import tpu as pltpu
from jax.sharding import PartitionSpec as P

MESH = pl.DeviceIdType.MESH
F32 = jnp.float32
BF16 = jnp.bfloat16


def nt(a, b):
    return lax.dot_general(a, b, (((1,), (1,)), ((), ())), preferred_element_type=F32)


def nn(a, b):
    return lax.dot_general(a, b, (((1,), (0,)), ((), ())), preferred_element_type=F32)


def wrap(i, n):
    return jnp.where(i >= n, i - n, i)


def split(x):
    high = x.astype(BF16)
    return high, (x - high.astype(F32)).astype(BF16)


def split3(x):
    high = x.astype(BF16)
    rest = x - high.astype(F32)
    middle = rest.astype(BF16)
    return high, middle, (rest - middle.astype(F32)).astype(BF16)


def rows_of(parts):
    return jnp.concatenate([x.astype(F32) for x in parts], axis=0).astype(BF16)


def exact(form, a, b):
    return lax.dot_general(
        a,
        b,
        (((1,), (0 if form is nn else 1,)), ((), ())),
        precision=lax.Precision.HIGHEST,
        preferred_element_type=F32,
    )


def product(form, a, b):
    ah, al = split(a)
    bh, bl = split(b)
    return form(ah, bh) + (form(ah, bl) + form(al, bh))


def eliminate(systems, n):
    state = [
        (a, [jnp.broadcast_to(a[:, first + j : first + j + 1], a.shape) for j in range(n)])
        for a, first in systems
    ]
    rows = lax.broadcasted_iota(jnp.int32, systems[0][0].shape, 0)
    for k in range(n):
        after = []
        for a, cols in state:
            pivot = cols[k]
            scale = 1.0 / pivot[k : k + 1, :]

            def update(x):
                row = x[k : k + 1, :] * scale
                return jnp.where(rows == k, row, x - pivot * row)

            after.append((update(a), [update(x) if j > k else x for j, x in enumerate(cols)]))
        state = after
    return [a for a, _ in state]


def kernel(
    cells,
    zs,
    chunks,
    rhs_hbm,
    near_hbm,
    neigh,
    up_hbm,
    su_hbm,
    far,
    tr_hbm,
    sd_hbm,
    dn_hbm,
    out,
    rhs,
    blocks,
    up,
    su,
    tr,
    sd,
    dn,
    ucat,
    gcat,
    pieces,
    halo0,
    halo1,
    mom0_out,
    mom0,
    momi_out,
    momi,
    loc_out,
    loc,
    gath_r,
    base,
    img,
    part_r,
    part_s,
    first,
    second,
    gram_out,
    grams,
    turned,
    near_sem,
    map_sem,
    h0_s,
    h0_r,
    m0_s,
    m0_r,
    gr_s,
    gr_r,
    pz_s,
    pz_r,
    lo_s,
    lo_r,
    g_s,
    g_r,
    mi_s,
    mi_r,
    h1_s,
    h1_r,
):
    c = lax.axis_index("patch")
    z = lax.axis_index("rhs")
    patches, cols, width = rhs.shape
    terms = su.shape[1]
    k = cols * zs
    total = patches * cells
    lists = far.shape[1]
    near_count = neigh.shape[0]

    maps = [(rhs_hbm, rhs), (up_hbm, up), (su_hbm, su), (sd_hbm, sd), (dn_hbm, dn), (tr_hbm, tr)]
    map_copies = [
        pltpu.make_async_copy(src, dst, map_sem.at[i]) for i, (src, dst) in enumerate(maps)
    ]

    def near_copy(p, rest):
        part = pl.ds(1, near_count - 1) if rest else pl.ds(0, 1)
        return pltpu.make_async_copy(
            near_hbm.at[p, part], blocks.at[p, part], near_sem.at[p, 1 if rest else 0]
        )

    for copy in map_copies[:3]:
        copy.start()
    barrier = pltpu.get_barrier_semaphore()

    def cell_of(i):
        return wrap(c + i, cells)

    def row_of(i):
        return wrap(z + i, zs)

    for i in range(1, cells):
        pl.semaphore_signal(barrier, inc=1, device_id=(cell_of(i), z), device_id_type=MESH)

    for i in range(1, zs):
        pl.semaphore_signal(barrier, inc=1, device_id=(c, row_of(i)), device_id_type=MESH)

    def below(i, body):
        pl.when(z >= i)(body)

    def above(i, body):
        pl.when(z < zs - i)(body)

    def send(src, dst, ssem, rsem, device):
        return pltpu.make_async_remote_copy(
            src_ref=src,
            dst_ref=dst,
            send_sem=ssem,
            recv_sem=rsem,
            device_id=device,
            device_id_type=MESH,
        )

    def piece_copy(target, slot):
        return send(
            pieces.at[1, z], pieces.at[1, slot], pz_s.at[target], pz_r.at[slot], (c, target)
        )

    def relay_copy(side, s):
        return send(
            pieces.at[1, s],
            pieces.at[2 * side, s],
            h0_s.at[side, s],
            h0_r.at[side, s],
            (cell_of(1 if side == 0 else cells - 1), z),
        )

    step = patches // chunks

    def halo1_copy(side, i):
        return send(
            halo1.at[pl.ds(patches + i * step, step)],
            halo1.at[pl.ds((0 if side == 0 else 2 * patches) + i * step, step)],
            h1_s.at[side, i],
            h1_r.at[side, i],
            (cell_of(1 if side == 0 else cells - 1), z),
        )

    def plane_copy(src, buf, ssem, rsem, target, slot):
        return send(src, buf.at[slot], ssem.at[target], rsem.at[slot], (target, z))

    def z_copy(src, buf, ssem, rsem, target, slot):
        return send(src, buf.at[slot], ssem.at[target], rsem.at[slot], (c, target))

    def plane(body):
        for i in range(1, cells):
            body(cell_of(i))

    def line(body):
        for i in range(1, zs):
            body(row_of(i))

    def moment0_copy(target, slot):
        return plane_copy(mom0_out, mom0, m0_s, m0_r, target, slot)

    def momenti_copy(target, slot):
        return plane_copy(momi_out, momi, mi_s, mi_r, target, slot)

    def gram_copy(it, target, slot):
        return plane_copy(gram_out.at[it], grams.at[it], g_s.at[it], g_r.at[it], target, slot)

    def rhs_copy(target, slot):
        return z_copy(rhs, gath_r, gr_s, gr_r, target, slot)

    def local_copy(target, slot):
        return z_copy(loc_out, loc, lo_s, lo_r, target, slot)

    map_copies[0].wait()
    for p in range(patches):
        near_copy(p, False).start()
    for p in range(patches):
        near_copy(p, True).start()
    for copy in map_copies[3:]:
        copy.start()
    for p in range(patches):
        pieces[1, z, p] = rhs[p].astype(BF16)
        gath_r[z, p] = rhs[p]

    pl.semaphore_wait(barrier, cells - 1 + zs - 1)
    for i in range(1, zs):
        below(i, lambda: piece_copy(z - i, z).start())
        above(i, lambda: piece_copy(z + i, z).start())
    relay_copy(0, z).start()
    relay_copy(1, z).start()

    map_copies[1].wait()
    map_copies[2].wait()
    acc = jnp.zeros((2 * cols, 2 * terms), F32)
    for p in range(patches):
        high, low = split(product(nn, su[p], up[p]))
        ucat[p, 0:terms, :] = high
        ucat[p, terms : 2 * terms, :] = low
        acc = acc + nt(rows_of(split(rhs[p])), ucat[p])
    acc = acc[0:cols] + acc[cols:]
    acc = acc[:, 0:terms] + acc[:, terms:]
    mom0_out[...] = jnp.concatenate([acc, jnp.zeros((cols, 128 - terms), F32)], axis=1)
    mom0[c] = mom0_out[...]
    plane(lambda t: moment0_copy(t, c).start())

    def pass_on(s):
        piece_copy(s, s).wait_recv()
        relay_copy(0, s).start()
        relay_copy(1, s).start()

    for i in range(1, zs):
        below(i, lambda: pass_on(z - i))
        above(i, lambda: pass_on(z + i))
        if i == 1:
            line(lambda t: rhs_copy(t, z).start())

    map_copies[5].wait()
    tall = jnp.concatenate([tr[0, j] for j in range(lists)], axis=1)

    def local_of(moments):
        wide = jnp.concatenate([moments[far[0, j]][:, 0:terms] for j in range(lists)], axis=1)
        return product(nt, wide, tall)

    plane(lambda s: moment0_copy(s, s).wait_recv())
    loc_out[...] = jnp.concatenate([local_of(mom0), jnp.zeros((cols, 128 - terms), F32)], axis=1)
    loc[z] = loc_out[...]
    line(lambda t: local_copy(t, z).start())

    def join(side):
        for p in range(patches):
            halo0[side * patches + p] = rows_of([pieces[side, s, p] for s in range(zs)])

    join(1)
    for p in range(patches):
        near_copy(p, False).wait()
    for p in range(patches):
        img[p] = nt(halo0[patches + p], blocks[p, 0])

    for copy in map_copies[3:5]:
        copy.wait()
    for p in range(patches):
        high, low = split(product(nn, sd[p].T, dn[p]))
        gcat[p, 0:terms, :] = high
        gcat[p, terms : 2 * terms, :] = low

    def far_of(local, p):
        high, low = split(local)
        both = jnp.concatenate(
            [jnp.concatenate([high, high], axis=1), jnp.concatenate([low, low], axis=1)], axis=0
        )
        both = nn(both, gcat[p])
        return both[0:k] + both[k:]

    def spot_of(p, j):
        spot = wrap(neigh[j, p] - (c * patches - patches) + total, total)
        return jnp.minimum(wrap(spot, total), 3 * patches - 1)

    for p in range(patches):
        near_copy(p, True).wait()
    for side in range(2):
        for s in range(zs):
            relay_copy(side, s).wait_recv()
        join(2 * side)
    for p in range(patches):
        acc = img[p]
        for j in range(1, near_count):
            acc = acc + nt(halo0[spot_of(p, j)], blocks[p, j])
        img[p] = acc

    line(lambda s: rhs_copy(s, s).wait_recv())
    for p in range(patches):
        for i, x in enumerate(split3(jnp.concatenate([gath_r[s, p] for s in range(zs)], axis=0))):
            first[p, 2 * i * k : (2 * i + 1) * k, :] = x

    line(lambda s: local_copy(s, s).wait_recv())
    local0 = jnp.concatenate([loc[s] for s in range(zs)], axis=0)[:, 0:terms]
    acc1 = jnp.zeros((4 * k, 2 * k), F32)
    acc2 = jnp.zeros((4 * k, 2 * k), F32)
    for p in range(patches):
        high, middle, low = split3(img[p] + far_of(local0, p))
        first[p, k : 2 * k, :] = high
        first[p, 3 * k : 4 * k, :] = middle
        first[p, 5 * k : 6 * k, :] = low
        one = jnp.concatenate([first[p, 0:k], high], axis=0)
        two = jnp.concatenate([first[p, 2 * k : 3 * k], middle], axis=0)
        both = jnp.concatenate([one, two], axis=0)
        acc1 = acc1 + nt(both, one)
        acc2 = acc2 + nt(both, two)
    gram = acc1[0 : 2 * k] + (acc1[2 * k :] + acc2[0 : 2 * k] + acc2[2 * k :])
    top, low = gram[0:k], gram[k:]
    gram_out[0] = jnp.concatenate(
        [
            0.5 * (top[:, k:] + low[:, 0:k]),
            top[:, 0:k],
            low,
            top,
            jnp.zeros((k, 128 - 6 * k), F32),
        ],
        axis=1,
    )
    grams[0, c] = gram_out[0]
    plane(lambda t: gram_copy(0, t, c).start())

    acc = jnp.zeros((2 * k, 2 * terms), F32)
    for p in range(patches):
        acc = acc + nt(
            jnp.concatenate([first[p, k : 2 * k], first[p, 3 * k : 4 * k]], axis=0), ucat[p]
        )
    acc = acc[0:k] + acc[k:]
    acc = acc[:, 0:terms] + acc[:, terms:]
    momi_out[...] = jnp.concatenate([acc, jnp.zeros((k, 128 - terms), F32)], axis=1)
    momi[c] = momi_out[...]
    plane(lambda t: momenti_copy(t, c).start())

    def collect(it):
        plane(lambda s: gram_copy(it, s, s).wait_recv())
        parts = [grams[it, i] for i in range(cells)]
        while len(parts) > 1:
            parts = [
                parts[i] + parts[i + 1] if i + 1 < len(parts) else parts[i]
                for i in range(0, len(parts), 2)
            ]
        return parts[0]

    eye = (
        lax.broadcasted_iota(jnp.int32, (k, k), 1) == lax.broadcasted_iota(jnp.int32, (k, k), 0)
    ).astype(F32)
    got = collect(0)
    one, two = eliminate([(got, 0), (got, 4 * k)], k)
    one_t, two_t = one.T, two.T
    alpha_t = one_t[k : 2 * k]
    beta1_t = (
        2.0 * eye
        - one_t[2 * k : 3 * k]
        + exact(nn, alpha_t, one_t[3 * k : 4 * k] - two_t[5 * k : 6 * k])
    )

    def doubled(x):
        high, low = split(x)
        high, low = high.astype(F32), low.astype(F32)
        return jnp.concatenate(
            [jnp.concatenate([high, high], axis=1), jnp.concatenate([low, low], axis=1)], axis=0
        ).astype(BF16)

    mixing = jnp.concatenate(
        [
            jnp.concatenate([x.astype(F32)] * 3, axis=1)
            for x in split3(jnp.concatenate([beta1_t, -alpha_t], axis=1))
        ],
        axis=0,
    ).astype(BF16)
    for p in range(patches):
        both = nn(mixing, first[p])
        high, low = split(both[0:k] + (both[k : 2 * k] + both[2 * k :]))
        halo1[patches + p] = high
        second[p, 0:k, :] = high
        second[p, k : 2 * k, :] = low
        if (p + 1) % step == 0:
            halo1_copy(0, p // step).start()
            halo1_copy(1, p // step).start()

    plane(lambda s: momenti_copy(s, s).wait_recv())
    local1 = product(nn, beta1_t, local0) - product(nn, alpha_t, local_of(momi))
    for p in range(patches):
        img[p] = nt(halo1[patches + p], blocks[p, 0]) + far_of(local1, p)
    mixed = exact(nt, got[:, 5 * k : 6 * k], alpha_t)
    new = (
        got[:, k : 2 * k]
        - mixed
        - mixed.T
        + exact(nn, alpha_t, exact(nt, got[:, 3 * k : 4 * k], alpha_t))
    )
    base[...] = jnp.zeros(base.shape, F32)
    base[:, k : 2 * k] = new
    right = base[...]
    turned[...] = one_t
    own = turned[pl.ds(k + z * cols, cols), :]
    high, low = [x.astype(F32) for x in split(own)]
    none = jnp.zeros_like(own)
    out_mix = jnp.concatenate(
        [
            jnp.concatenate([high, none, high, none], axis=1),
            jnp.concatenate([low, none, low, none], axis=1),
            jnp.concatenate([none, high, none, high], axis=1),
            jnp.concatenate([none, low, none, low], axis=1),
        ],
        axis=0,
    ).astype(BF16)
    for p in range(patches):
        both = nn(out_mix, first[p, 0 : 4 * k])
        part_s[p] = both[0:cols] + both[cols : 2 * cols]
        part_r[p] = rhs[p] - (both[2 * cols : 3 * cols] + both[3 * cols :])

    for i in range(chunks):
        halo1_copy(0, i).wait_recv()
        halo1_copy(1, i).wait_recv()
    acc1 = jnp.zeros((2 * k, k), F32)
    acc2 = jnp.zeros((k, k), F32)
    for p in range(patches):
        acc = img[p]
        for j in range(1, near_count):
            acc = acc + nt(halo1[spot_of(p, j)], blocks[p, j])
        high, low = split(acc)
        second[p, 2 * k : 3 * k, :] = high
        second[p, 3 * k : 4 * k, :] = low
        acc1 = acc1 + nt(second[p, 0 : 2 * k], high)
        acc2 = acc2 + nt(second[p, 0:k], low)
    curve = acc1[0:k] + acc1[k:] + acc2
    gram_out[1] = jnp.concatenate(
        [0.5 * (curve + curve.T), jnp.zeros((k, 128 - k), F32)], axis=1
    )
    grams[1, c] = gram_out[1]
    plane(lambda t: gram_copy(1, t, c).start())
    (last,) = eliminate([(collect(1) + right, 0)], k)
    turned[...] = last.T
    out_mix = doubled(turned[pl.ds(k + z * cols, cols), :])
    for p in range(patches):
        both = nn(out_mix, second[p, 0 : 2 * k])
        out[p, 0:cols, :] = part_s[p] + (both[0:cols] + both[cols:])
        both = nn(out_mix, second[p, 2 * k : 4 * k])
        out[p, cols : 2 * cols, :] = part_r[p] - (both[0:cols] + both[cols:])

    for side in range(2):
        for s in range(zs):
            relay_copy(side, s).wait_send()
        for i in range(chunks):
            halo1_copy(side, i).wait_send()
    line(lambda t: piece_copy(t, z).wait_send())
    line(lambda t: rhs_copy(t, z).wait_send())
    line(lambda t: local_copy(t, z).wait_send())
    plane(lambda t: moment0_copy(t, c).wait_send())
    plane(lambda t: momenti_copy(t, c).wait_send())
    for it in range(2):
        plane(lambda t, it=it: gram_copy(it, t, c).wait_send())


def on_device(cells, zs, *args):
    rhs, near, neigh, up, su, far, tr, sd, dn = args
    patches, cols, width = rhs.shape
    terms = su.shape[1]
    dn = jnp.swapaxes(dn, 1, 2)
    neigh = neigh.T
    k = cols * zs
    chunks = 4 if patches % 4 == 0 else 1
    vmem = pl.BlockSpec(memory_space=pltpu.VMEM)
    smem = pl.BlockSpec(memory_space=pltpu.SMEM)
    hbm = pl.BlockSpec(memory_space=pltpu.HBM)
    dma = pltpu.SemaphoreType.DMA
    out = pl.pallas_call(
        functools.partial(kernel, cells, zs, chunks),
        out_shape=pltpu.VMEM((patches, 2 * cols, width), F32),
        in_specs=[hbm, hbm, smem, hbm, hbm, smem, hbm, hbm, hbm],
        out_specs=vmem,
        scratch_shapes=[
            pltpu.VMEM(rhs.shape, F32),
            pltpu.VMEM(near.shape, near.dtype),
            pltpu.VMEM(up.shape, F32),
            pltpu.VMEM(su.shape, F32),
            pltpu.VMEM(tr.shape, F32),
            pltpu.VMEM(sd.shape, F32),
            pltpu.VMEM(dn.shape, F32),
            pltpu.VMEM((patches, 2 * terms, width), BF16),
            pltpu.VMEM((patches, 2 * terms, width), BF16),
            pltpu.VMEM((3, zs) + rhs.shape, BF16),
            pltpu.VMEM((3 * patches, k, width), BF16),
            pltpu.VMEM((3 * patches, k, width), BF16),
            pltpu.VMEM((cols, 128), F32),
            pltpu.VMEM((cells, cols, 128), F32),
            pltpu.VMEM((k, 128), F32),
            pltpu.VMEM((cells, k, 128), F32),
            pltpu.VMEM((cols, 128), F32),
            pltpu.VMEM((zs, cols, 128), F32),
            pltpu.VMEM((zs,) + rhs.shape, F32),
            pltpu.VMEM((k, 128), F32),
            pltpu.VMEM((patches, k, width), F32),
            pltpu.VMEM(rhs.shape, F32),
            pltpu.VMEM(rhs.shape, F32),
            pltpu.VMEM((patches, 6 * k, width), BF16),
            pltpu.VMEM((patches, 4 * k, width), BF16),
            pltpu.VMEM((2, k, 128), F32),
            pltpu.VMEM((2, cells, k, 128), F32),
            pltpu.VMEM((128, k), F32),
            dma((patches, 2)),
            dma((6,)),
            dma((2, zs)),
            dma((2, zs)),
            dma((cells,)),
            dma((cells,)),
            dma((zs,)),
            dma((zs,)),
            dma((zs,)),
            dma((zs,)),
            dma((zs,)),
            dma((zs,)),
            dma((2, cells)),
            dma((2, cells)),
            dma((cells,)),
            dma((cells,)),
            dma((2, chunks)),
            dma((2, chunks)),
        ],
        compiler_params=pltpu.CompilerParams(
            collective_id=0, has_side_effects=True, vmem_limit_bytes=60 * 1024 * 1024
        ),
        name="block_cg",
    )(rhs, near, neigh, up, su, far, tr, sd, dn)
    return out[:, 0:cols], out[:, cols:]


def solution(mesh):
    cells = mesh.shape["patch"]
    zs = mesh.shape["rhs"]
    return jax.shard_map(
        functools.partial(on_device, cells, zs),
        mesh=mesh,
        in_specs=(
            P("patch", "rhs", None),
            P("patch", None, None, None),
            P("patch", None),
            P("patch", None, None),
            P("patch", None, None),
            P("patch", None),
            P("patch", None, None, None),
            P("patch", None, None),
            P("patch", None, None),
        ),
        out_specs=(P("patch", "rhs", None), P("patch", "rhs", None)),
        check_vma=False,
    )
```

```python
import functools

import jax
import jax.numpy as jnp
from jax import lax
from jax.experimental import pallas as pl
from jax.experimental.pallas import tpu as pltpu
from jax.sharding import PartitionSpec as P

MESH = pl.DeviceIdType.MESH
F32 = jnp.float32
BF16 = jnp.bfloat16


def nt(a, b):
    return lax.dot_general(a, b, (((1,), (1,)), ((), ())), preferred_element_type=F32)


def nn(a, b):
    return lax.dot_general(a, b, (((1,), (0,)), ((), ())), preferred_element_type=F32)


def wrap(i, n):
    return jnp.where(i >= n, i - n, i)


def split(x):
    high = x.astype(BF16)
    return high, (x - high.astype(F32)).astype(BF16)


def split3(x):
    high = x.astype(BF16)
    rest = x - high.astype(F32)
    middle = rest.astype(BF16)
    return high, middle, (rest - middle.astype(F32)).astype(BF16)


def rows_of(parts):
    return jnp.concatenate([x.astype(F32) for x in parts], axis=0).astype(BF16)


def exact(form, a, b):
    return lax.dot_general(
        a,
        b,
        (((1,), (0 if form is nn else 1,)), ((), ())),
        precision=lax.Precision.HIGHEST,
        preferred_element_type=F32,
    )


def product(form, a, b):
    ah, al = split(a)
    bh, bl = split(b)
    return form(ah, bh) + (form(ah, bl) + form(al, bh))


def eliminate(systems, n):
    state = [
        (a, [jnp.broadcast_to(a[:, first + j : first + j + 1], a.shape) for j in range(n)])
        for a, first in systems
    ]
    rows = lax.broadcasted_iota(jnp.int32, systems[0][0].shape, 0)
    for k in range(n):
        after = []
        for a, cols in state:
            pivot = cols[k]
            scale = 1.0 / pivot[k : k + 1, :]

            def update(x):
                row = x[k : k + 1, :] * scale
                return jnp.where(rows == k, row, x - pivot * row)

            after.append((update(a), [update(x) if j > k else x for j, x in enumerate(cols)]))
        state = after
    return [a for a, _ in state]


def kernel(
    cells,
    zs,
    chunks,
    rhs_hbm,
    near_hbm,
    neigh,
    up_hbm,
    su_hbm,
    far,
    tr_hbm,
    sd_hbm,
    dn_hbm,
    out,
    rhs,
    blocks,
    up,
    su,
    tr,
    sd,
    dn,
    ucat,
    gcat,
    pieces,
    halo0,
    halo1,
    mom0_out,
    mom0,
    momi_out,
    momi,
    loc_out,
    loc,
    gath_r,
    base,
    img,
    part_r,
    part_s,
    first,
    second,
    gram_out,
    grams,
    turned,
    near_sem,
    map_sem,
    h0_s,
    h0_r,
    m0_s,
    m0_r,
    gr_s,
    gr_r,
    pz_s,
    pz_r,
    lo_s,
    lo_r,
    g_s,
    g_r,
    mi_s,
    mi_r,
    h1_s,
    h1_r,
):
    c = lax.axis_index("patch")
    z = lax.axis_index("rhs")
    patches, cols, width = rhs.shape
    terms = su.shape[1]
    k = cols * zs
    total = patches * cells
    lists = far.shape[1]
    near_count = neigh.shape[0]

    maps = [(rhs_hbm, rhs), (up_hbm, up), (su_hbm, su), (sd_hbm, sd), (dn_hbm, dn), (tr_hbm, tr)]
    map_copies = [
        pltpu.make_async_copy(src, dst, map_sem.at[i]) for i, (src, dst) in enumerate(maps)
    ]

    def near_copy(p, rest):
        part = pl.ds(1, near_count - 1) if rest else pl.ds(0, 1)
        return pltpu.make_async_copy(
            near_hbm.at[p, part], blocks.at[p, part], near_sem.at[p, 1 if rest else 0]
        )

    for copy in map_copies[:3]:
        copy.start()
    barrier = pltpu.get_barrier_semaphore()

    def cell_of(i):
        return wrap(c + i, cells)

    def row_of(i):
        return wrap(z + i, zs)

    for i in range(1, cells):
        pl.semaphore_signal(barrier, inc=1, device_id=(cell_of(i), z), device_id_type=MESH)

    for i in range(1, zs):
        pl.semaphore_signal(barrier, inc=1, device_id=(c, row_of(i)), device_id_type=MESH)

    def below(i, body):
        pl.when(z >= i)(body)

    def above(i, body):
        pl.when(z < zs - i)(body)

    def send(src, dst, ssem, rsem, device):
        return pltpu.make_async_remote_copy(
            src_ref=src,
            dst_ref=dst,
            send_sem=ssem,
            recv_sem=rsem,
            device_id=device,
            device_id_type=MESH,
        )

    def piece_copy(target, slot):
        return send(
            pieces.at[1, z], pieces.at[1, slot], pz_s.at[target], pz_r.at[slot], (c, target)
        )

    def relay_copy(side, s):
        return send(
            pieces.at[1, s],
            pieces.at[2 * side, s],
            h0_s.at[side, s],
            h0_r.at[side, s],
            (cell_of(1 if side == 0 else cells - 1), z),
        )

    step = patches // chunks

    def halo1_copy(side, i):
        return send(
            halo1.at[pl.ds(patches + i * step, step)],
            halo1.at[pl.ds((0 if side == 0 else 2 * patches) + i * step, step)],
            h1_s.at[side, i],
            h1_r.at[side, i],
            (cell_of(1 if side == 0 else cells - 1), z),
        )

    def plane_copy(src, buf, ssem, rsem, target, slot):
        return send(src, buf.at[slot], ssem.at[target], rsem.at[slot], (target, z))

    def z_copy(src, buf, ssem, rsem, target, slot):
        return send(src, buf.at[slot], ssem.at[target], rsem.at[slot], (c, target))

    def plane(body):
        for i in range(1, cells):
            body(cell_of(i))

    def line(body):
        for i in range(1, zs):
            body(row_of(i))

    def moment0_copy(target, slot):
        return plane_copy(mom0_out, mom0, m0_s, m0_r, target, slot)

    def momenti_copy(target, slot):
        return plane_copy(momi_out, momi, mi_s, mi_r, target, slot)

    def gram_copy(it, target, slot):
        return plane_copy(gram_out.at[it], grams.at[it], g_s.at[it], g_r.at[it], target, slot)

    def rhs_copy(target, slot):
        return z_copy(rhs, gath_r, gr_s, gr_r, target, slot)

    def local_copy(target, slot):
        return z_copy(loc_out, loc, lo_s, lo_r, target, slot)

    map_copies[0].wait()
    for p in range(patches):
        near_copy(p, False).start()
    for p in range(patches):
        near_copy(p, True).start()
    for copy in map_copies[3:]:
        copy.start()
    for p in range(patches):
        pieces[1, z, p] = rhs[p].astype(BF16)
        gath_r[z, p] = rhs[p]

    pl.semaphore_wait(barrier, cells - 1 + zs - 1)
    for i in range(1, zs):
        below(i, lambda: piece_copy(z - i, z).start())
        above(i, lambda: piece_copy(z + i, z).start())
    relay_copy(0, z).start()
    relay_copy(1, z).start()

    map_copies[1].wait()
    map_copies[2].wait()
    acc = jnp.zeros((2 * cols, 2 * terms), F32)
    for p in range(patches):
        high, low = split(product(nn, su[p], up[p]))
        ucat[p, 0:terms, :] = high
        ucat[p, terms : 2 * terms, :] = low
    for p in range(patches):
        acc = acc + nt(rows_of(split(rhs[p])), ucat[p])
    acc = acc[0:cols] + acc[cols:]
    acc = acc[:, 0:terms] + acc[:, terms:]
    mom0_out[...] = jnp.concatenate([acc, jnp.zeros((cols, 128 - terms), F32)], axis=1)
    mom0[c] = mom0_out[...]
    plane(lambda t: moment0_copy(t, c).start())

    def pass_on(s):
        piece_copy(s, s).wait_recv()
        relay_copy(0, s).start()
        relay_copy(1, s).start()

    for i in range(1, zs):
        below(i, lambda: pass_on(z - i))
        above(i, lambda: pass_on(z + i))
        if i == 1:
            line(lambda t: rhs_copy(t, z).start())

    map_copies[5].wait()
    tall = jnp.concatenate([tr[0, j] for j in range(lists)], axis=1)

    def local_of(moments):
        wide = jnp.concatenate([moments[far[0, j]][:, 0:terms] for j in range(lists)], axis=1)
        return product(nt, wide, tall)

    plane(lambda s: moment0_copy(s, s).wait_recv())
    loc_out[...] = jnp.concatenate([local_of(mom0), jnp.zeros((cols, 128 - terms), F32)], axis=1)
    loc[z] = loc_out[...]
    line(lambda t: local_copy(t, z).start())

    def join(side):
        for p in range(patches):
            halo0[side * patches + p] = rows_of([pieces[side, s, p] for s in range(zs)])

    join(1)
    for p in range(patches):
        near_copy(p, False).wait()
    for p in range(patches):
        img[p] = nt(halo0[patches + p], blocks[p, 0])

    for copy in map_copies[3:5]:
        copy.wait()
    for p in range(patches):
        high, low = split(product(nn, sd[p].T, dn[p]))
        gcat[p, 0:terms, :] = high
        gcat[p, terms : 2 * terms, :] = low

    def far_of(local, p):
        high, low = split(local)
        both = jnp.concatenate(
            [jnp.concatenate([high, high], axis=1), jnp.concatenate([low, low], axis=1)], axis=0
        )
        both = nn(both, gcat[p])
        return both[0:k] + both[k:]

    def spot_of(p, j):
        spot = wrap(neigh[j, p] - (c * patches - patches) + total, total)
        return jnp.minimum(wrap(spot, total), 3 * patches - 1)

    for p in range(patches):
        near_copy(p, True).wait()
    for side in range(2):
        for s in range(zs):
            relay_copy(side, s).wait_recv()
        join(2 * side)
    for p in range(patches):
        acc = img[p]
        for j in range(1, near_count):
            acc = acc + nt(halo0[spot_of(p, j)], blocks[p, j])
        img[p] = acc

    line(lambda s: rhs_copy(s, s).wait_recv())
    for p in range(patches):
        for i, x in enumerate(split3(jnp.concatenate([gath_r[s, p] for s in range(zs)], axis=0))):
            first[p, 2 * i * k : (2 * i + 1) * k, :] = x

    line(lambda s: local_copy(s, s).wait_recv())
    local0 = jnp.concatenate([loc[s] for s in range(zs)], axis=0)[:, 0:terms]
    for p in range(patches):
        img[p] += far_of(local0, p)
    acc1 = jnp.zeros((4 * k, 2 * k), F32)
    acc2 = jnp.zeros((4 * k, 2 * k), F32)
    for p in range(patches):
        for i, x in enumerate(split3(img[p])):
            first[p, (2 * i + 1) * k : (2 * i + 2) * k, :] = x
    for p in range(patches):
        acc1 = acc1 + nt(first[p, 0 : 4 * k], first[p, 0 : 2 * k])
    for p in range(patches):
        acc2 = acc2 + nt(first[p, 0 : 4 * k], first[p, 2 * k : 4 * k])
    gram = acc1[0 : 2 * k] + (acc1[2 * k :] + acc2[0 : 2 * k] + acc2[2 * k :])
    top, low = gram[0:k], gram[k:]
    gram_out[0] = jnp.concatenate(
        [
            0.5 * (top[:, k:] + low[:, 0:k]),
            top[:, 0:k],
            low,
            top,
            jnp.zeros((k, 128 - 6 * k), F32),
        ],
        axis=1,
    )
    grams[0, c] = gram_out[0]
    plane(lambda t: gram_copy(0, t, c).start())

    acc = jnp.zeros((2 * k, 2 * terms), F32)
    for p in range(patches):
        acc = acc + nt(
            jnp.concatenate([first[p, k : 2 * k], first[p, 3 * k : 4 * k]], axis=0), ucat[p]
        )
    acc = acc[0:k] + acc[k:]
    acc = acc[:, 0:terms] + acc[:, terms:]
    momi_out[...] = jnp.concatenate([acc, jnp.zeros((k, 128 - terms), F32)], axis=1)
    momi[c] = momi_out[...]
    plane(lambda t: momenti_copy(t, c).start())

    def collect(it):
        plane(lambda s: gram_copy(it, s, s).wait_recv())
        parts = [grams[it, i] for i in range(cells)]
        while len(parts) > 1:
            parts = [
                parts[i] + parts[i + 1] if i + 1 < len(parts) else parts[i]
                for i in range(0, len(parts), 2)
            ]
        return parts[0]

    eye = (
        lax.broadcasted_iota(jnp.int32, (k, k), 1) == lax.broadcasted_iota(jnp.int32, (k, k), 0)
    ).astype(F32)
    got = collect(0)
    one, two = eliminate([(got, 0), (got, 4 * k)], k)
    one_t, two_t = one.T, two.T
    alpha_t = one_t[k : 2 * k]
    beta1_t = (
        2.0 * eye
        - one_t[2 * k : 3 * k]
        + exact(nn, alpha_t, one_t[3 * k : 4 * k] - two_t[5 * k : 6 * k])
    )

    def doubled(x):
        high, low = split(x)
        high, low = high.astype(F32), low.astype(F32)
        return jnp.concatenate(
            [jnp.concatenate([high, high], axis=1), jnp.concatenate([low, low], axis=1)], axis=0
        ).astype(BF16)

    mixing = jnp.concatenate(
        [
            jnp.concatenate([x.astype(F32)] * 3, axis=1)
            for x in split3(jnp.concatenate([beta1_t, -alpha_t], axis=1))
        ],
        axis=0,
    ).astype(BF16)
    for p in range(patches):
        both = nn(mixing, first[p])
        high, low = split(both[0:k] + (both[k : 2 * k] + both[2 * k :]))
        halo1[patches + p] = high
        second[p, 0:k, :] = high
        second[p, k : 2 * k, :] = low
        if (p + 1) % step == 0:
            halo1_copy(0, p // step).start()
            halo1_copy(1, p // step).start()

    plane(lambda s: momenti_copy(s, s).wait_recv())
    local1 = product(nn, beta1_t, local0) - product(nn, alpha_t, local_of(momi))
    for p in range(patches):
        img[p] = nt(halo1[patches + p], blocks[p, 0])
    for p in range(patches):
        img[p] += far_of(local1, p)
    for i in range(chunks):
        halo1_copy(0, i).wait_recv()
        halo1_copy(1, i).wait_recv()
    for p in range(patches):
        acc = img[p]
        for j in range(1, near_count):
            acc = acc + nt(halo1[spot_of(p, j)], blocks[p, j])
        img[p] = acc
    acc1 = jnp.zeros((2 * k, k), F32)
    acc2 = jnp.zeros((k, k), F32)
    for p in range(patches):
        high, low = split(img[p])
        second[p, 2 * k : 3 * k, :] = high
        second[p, 3 * k : 4 * k, :] = low
        acc1 = acc1 + nt(second[p, 0 : 2 * k], high)
        acc2 = acc2 + nt(second[p, 0:k], low)
    curve = acc1[0:k] + acc1[k:] + acc2
    gram_out[1] = jnp.concatenate(
        [0.5 * (curve + curve.T), jnp.zeros((k, 128 - k), F32)], axis=1
    )
    grams[1, c] = gram_out[1]
    plane(lambda t: gram_copy(1, t, c).start())
    mixed = exact(nt, got[:, 5 * k : 6 * k], alpha_t)
    new = (
        got[:, k : 2 * k]
        - mixed
        - mixed.T
        + exact(nn, alpha_t, exact(nt, got[:, 3 * k : 4 * k], alpha_t))
    )
    base[...] = jnp.zeros(base.shape, F32)
    base[:, k : 2 * k] = new
    right = base[...]
    turned[...] = one_t
    own = turned[pl.ds(k + z * cols, cols), :]
    high, low = [x.astype(F32) for x in split(own)]
    none = jnp.zeros_like(own)
    out_mix = jnp.concatenate(
        [
            jnp.concatenate([high, none, high, none], axis=1),
            jnp.concatenate([low, none, low, none], axis=1),
            jnp.concatenate([none, high, none, high], axis=1),
            jnp.concatenate([none, low, none, low], axis=1),
        ],
        axis=0,
    ).astype(BF16)
    for p in range(patches):
        both = nn(out_mix, first[p, 0 : 4 * k])
        part_s[p] = both[0:cols] + both[cols : 2 * cols]
        part_r[p] = rhs[p] - (both[2 * cols : 3 * cols] + both[3 * cols :])

    (last,) = eliminate([(collect(1) + right, 0)], k)
    turned[...] = last.T
    out_mix = doubled(turned[pl.ds(k + z * cols, cols), :])
    for p in range(patches):
        both = nn(out_mix, second[p, 0 : 2 * k])
        out[p, 0:cols, :] = part_s[p] + (both[0:cols] + both[cols:])
        both = nn(out_mix, second[p, 2 * k : 4 * k])
        out[p, cols : 2 * cols, :] = part_r[p] - (both[0:cols] + both[cols:])

    for side in range(2):
        for s in range(zs):
            relay_copy(side, s).wait_send()
        for i in range(chunks):
            halo1_copy(side, i).wait_send()
    line(lambda t: piece_copy(t, z).wait_send())
    line(lambda t: rhs_copy(t, z).wait_send())
    line(lambda t: local_copy(t, z).wait_send())
    plane(lambda t: moment0_copy(t, c).wait_send())
    plane(lambda t: momenti_copy(t, c).wait_send())
    for it in range(2):
        plane(lambda t, it=it: gram_copy(it, t, c).wait_send())


def on_device(cells, zs, *args):
    rhs, near, neigh, up, su, far, tr, sd, dn = args
    patches, cols, width = rhs.shape
    terms = su.shape[1]
    dn = jnp.swapaxes(dn, 1, 2)
    neigh = neigh.T
    k = cols * zs
    chunks = 4 if patches % 4 == 0 else 1
    vmem = pl.BlockSpec(memory_space=pltpu.VMEM)
    smem = pl.BlockSpec(memory_space=pltpu.SMEM)
    hbm = pl.BlockSpec(memory_space=pltpu.HBM)
    dma = pltpu.SemaphoreType.DMA
    out = pl.pallas_call(
        functools.partial(kernel, cells, zs, chunks),
        out_shape=pltpu.VMEM((patches, 2 * cols, width), F32),
        in_specs=[hbm, hbm, smem, hbm, hbm, smem, hbm, hbm, hbm],
        out_specs=vmem,
        scratch_shapes=[
            pltpu.VMEM(rhs.shape, F32),
            pltpu.VMEM(near.shape, near.dtype),
            pltpu.VMEM(up.shape, F32),
            pltpu.VMEM(su.shape, F32),
            pltpu.VMEM(tr.shape, F32),
            pltpu.VMEM(sd.shape, F32),
            pltpu.VMEM(dn.shape, F32),
            pltpu.VMEM((patches, 2 * terms, width), BF16),
            pltpu.VMEM((patches, 2 * terms, width), BF16),
            pltpu.VMEM((3, zs) + rhs.shape, BF16),
            pltpu.VMEM((3 * patches, k, width), BF16),
            pltpu.VMEM((3 * patches, k, width), BF16),
            pltpu.VMEM((cols, 128), F32),
            pltpu.VMEM((cells, cols, 128), F32),
            pltpu.VMEM((k, 128), F32),
            pltpu.VMEM((cells, k, 128), F32),
            pltpu.VMEM((cols, 128), F32),
            pltpu.VMEM((zs, cols, 128), F32),
            pltpu.VMEM((zs,) + rhs.shape, F32),
            pltpu.VMEM((k, 128), F32),
            pltpu.VMEM((patches, k, width), F32),
            pltpu.VMEM(rhs.shape, F32),
            pltpu.VMEM(rhs.shape, F32),
            pltpu.VMEM((patches, 6 * k, width), BF16),
            pltpu.VMEM((patches, 4 * k, width), BF16),
            pltpu.VMEM((2, k, 128), F32),
            pltpu.VMEM((2, cells, k, 128), F32),
            pltpu.VMEM((128, k), F32),
            dma((patches, 2)),
            dma((6,)),
            dma((2, zs)),
            dma((2, zs)),
            dma((cells,)),
            dma((cells,)),
            dma((zs,)),
            dma((zs,)),
            dma((zs,)),
            dma((zs,)),
            dma((zs,)),
            dma((zs,)),
            dma((2, cells)),
            dma((2, cells)),
            dma((cells,)),
            dma((cells,)),
            dma((2, chunks)),
            dma((2, chunks)),
        ],
        compiler_params=pltpu.CompilerParams(
            collective_id=0, has_side_effects=True, vmem_limit_bytes=60 * 1024 * 1024
        ),
        name="block_cg",
    )(rhs, near, neigh, up, su, far, tr, sd, dn)
    return out[:, 0:cols], out[:, cols:]


def solution(mesh):
    cells = mesh.shape["patch"]
    zs = mesh.shape["rhs"]
    return jax.shard_map(
        functools.partial(on_device, cells, zs),
        mesh=mesh,
        in_specs=(
            P("patch", "rhs", None),
            P("patch", None, None, None),
            P("patch", None),
            P("patch", None, None),
            P("patch", None, None),
            P("patch", None),
            P("patch", None, None, None),
            P("patch", None, None),
            P("patch", None, None),
        ),
        out_specs=(P("patch", "rhs", None), P("patch", "rhs", None)),
        check_vma=False,
    )
```
